256 devices in a mesh: dp: 64 (over y, z, core), neg: 4 (over x).
Axes of the slice: x: 4, y: 4, z: 8, core: 2. Of those that a mesh axis runs over, the one named last changes fastest.
Arguments:
- user_embed: bfloat16 [196608, 256], P(('dp', 'neg')), may hold values from -25 to 25
- positive_embed: bfloat16 [196608, 256], P(('dp', 'neg')), may hold values from -6 to 6
- positive_ids: int32 [196608], P(('dp', 'neg')), may hold values from 0 to 1048575
- token_weights: int32 [196608], P(('dp', 'neg')), may hold values from 1 to 5
- offsets: int32 [64, 25], P('dp'), may hold values from 0 to 3072, as said below
- negative_embed: bfloat16 [32768, 256], P('neg'), may hold values from -6 to 6
- negative_ids: int32 [32768], P('neg'), may hold values from 0 to 1048575
Outputs:
- token_loss: float32 [196608], P(('dp', 'neg'))
- mean_loss: float32 [], replicated
The draws below stay inside these ranges and needn't reach their ends.
Inputs may be any that keep to these rules, and one draw needn't show every extreme that they name: `offsets`: each row starts at 0 and does not fall; every user holds 2 or more slots; in every draw some group fills all 3072 slots.
All inputs are finite; a program needn't handle non-finite values.
Results may differ from the reference program's by a relative error of at most 0.0003.
Values may be sent and summed in bfloat16 or wider, within the bound.
A program may use at most 64 MiB of HBM per device.

```python
import math
import jax
import jax.numpy as jnp
from jax import lax

D = 256
NEG_DEV = 8192
TOK_DEV = 768
USERS = 24
ITEMS = 1048576
NEGS = 32768
TOKENS = 196608
N_DP = 64
N_NEG = 4


def drawn_slots(key):
    base = jax.random.fold_in(key, 13)
    chosen = jax.random.permutation(jax.random.fold_in(base, 1), NEGS // 2)[:32].astype(jnp.int32)
    picked = (2 * NEG_DEV * (chosen // NEG_DEV) + chosen % NEG_DEV).astype(jnp.int32)
    partner = (picked + NEG_DEV).astype(jnp.int32)
    strengths = jax.random.uniform(jax.random.fold_in(base, 2), (32,), jnp.float32, 6.0, 10.0)
    targets = jax.random.permutation(jax.random.fold_in(base, 3), TOKENS)[:32].astype(jnp.int32)
    return (picked, partner, strengths, targets)


def negative_table(key):
    base = jax.random.fold_in(key, 11)
    table = jnp.clip(jax.random.normal(base, (NEGS, D), jnp.float32), -6.0, 6.0)
    return table


def draw_negative_embed(key, part):
    return negative_table(key).astype(jnp.bfloat16)


def draw_user_embed(key, part):
    base = jax.random.fold_in(key, 17)
    table = negative_table(key)
    picked, partner, strengths, targets = drawn_slots(key)
    rows = jnp.clip(jax.random.normal(base, (TOKENS, D), jnp.float32), -6.0, 6.0)
    rows = rows.at[targets].set(0.25 * strengths[:, None] * table[picked])
    return rows.astype(jnp.bfloat16)


def item_ids(key, salt, number):
    mixing = jax.random.fold_in(key, 5)
    factor = jax.random.randint(jax.random.fold_in(mixing, 1), (), 0, 1024) * 2 + 1
    offset = jax.random.randint(jax.random.fold_in(mixing, 2), (), 0, ITEMS)
    base = jax.random.fold_in(key, salt)
    levels = jax.random.randint(jax.random.fold_in(base, 1), (number,), 0, 21)
    upper = jnp.left_shift(jnp.ones((number,), jnp.int32), levels)
    raw = jax.random.randint(jax.random.fold_in(base, 2), (number,), 0, upper)
    return jnp.bitwise_and(raw * factor + offset, ITEMS - 1).astype(jnp.int32)


def draw_positive_ids(key, part):
    return item_ids(key, 21, TOKENS)


def draw_negative_ids(key, part):
    values = item_ids(key, 23, NEGS)
    picked, partner, strengths, targets = drawn_slots(key)
    wanted = item_ids(key, 21, TOKENS)[targets[:16]]
    values = values.at[picked[:16]].set(wanted)
    values = values.at[partner[:16]].set(wanted)
    return values.astype(jnp.int32)


def draw_offsets(key, part):
    base = jax.random.fold_in(key, 29)
    group_size = TOK_DEV * N_NEG
    groups = jnp.arange(N_DP, dtype=jnp.int32)
    start_live = group_size * (N_DP + 2 * groups) // (3 * N_DP)
    jitter = jax.random.randint(jax.random.fold_in(base, 1), (N_DP,), 0, group_size // 16 + 1)
    live = jnp.maximum(start_live - jitter, 2 * USERS)
    filled = jax.random.randint(jax.random.fold_in(base, 2), (), 0, N_DP)
    live = jnp.where(groups == filled, group_size, live)
    cuts = jax.random.randint(jax.random.fold_in(base, 3), (N_DP, USERS - 1), 0, (live - 2 * USERS + 1)[:, None])
    cuts = jnp.sort(cuts, axis=1)
    middle = cuts + 2 * jnp.arange(1, USERS, dtype=jnp.int32)[None, :]
    zeros_col = jnp.zeros((N_DP, 1), jnp.int32)
    return jnp.concatenate([zeros_col, middle, live[:, None]], axis=1).astype(jnp.int32)


def with_ends(drawn, key, smallest, top_value):
    longest = drawn.shape.index(max(drawn.shape))
    spots = []
    for shift in (0, 1):
        where = [jax.random.randint(jax.random.fold_in(key, axis), (), 0, length) for axis, length in enumerate(drawn.shape)]
        where[longest] = (where[longest] + shift) % drawn.shape[longest]
        spots.append(tuple(where))
    return drawn.at[spots[0]].set(smallest).at[spots[1]].set(top_value)


def block_scale(key, extent, cuts, smallest, largest):
    level = 1.0
    for position, shards_of in cuts:
        draws = jax.random.uniform(jax.random.fold_in(jax.random.fold_in(key, 6), position), (shards_of,), jnp.float32, smallest / len(cuts), largest / len(cuts))
        level = level * jnp.repeat(jnp.exp(draws), extent[position] // shards_of).reshape((-1,) + (1,) * (len(extent) - 1 - position))
    return level


def scatter_about(rng, shape, spread, most, pieces=(), kind=jnp.bfloat16):
    values = jax.random.normal(rng, shape, jnp.float32) * spread
    if len(pieces) > 0:
        values = block_scale(rng, shape, pieces, -0.22, 0.18) * values
    return jnp.clip(values, min=-most, max=most).astype(kind)


def setup_inputs(seed: int = 0) -> dict:
    arg_keys = jax.random.split(jax.random.key(seed), 8)
    return {
        "user_embed": draw_user_embed(jax.random.fold_in(arg_keys[7], 71), 0),
        "positive_embed": scatter_about(arg_keys[1], (TOKENS, D), 1.0, 6.0, ((0, 256),)),
        "positive_ids": draw_positive_ids(jax.random.fold_in(arg_keys[7], 71), 0),
        "token_weights": with_ends(jax.random.randint(arg_keys[3], (TOKENS,), 1, 6), jax.random.fold_in(arg_keys[3], 1), 1, 5).astype(jnp.int32),
        "offsets": draw_offsets(jax.random.fold_in(arg_keys[7], 71), 0),
        "negative_embed": draw_negative_embed(jax.random.fold_in(arg_keys[7], 71), 0),
        "negative_ids": draw_negative_ids(jax.random.fold_in(arg_keys[7], 71), 0),
    }


def reference(user_embed, positive_embed, positive_ids, token_weights, offsets, negative_embed, negative_ids):
    scale = 3.0 / math.sqrt(D)
    block = math.gcd(TOKENS, 512)
    users_blocks = user_embed.reshape(TOKENS // block, block, D)
    pos_blocks = positive_embed.reshape(TOKENS // block, block, D)
    ids_blocks = positive_ids.reshape(TOKENS // block, block)

    def one_block(triple):
        rows, pos_rows, row_ids = triple
        logits = jnp.dot(rows, negative_embed.T, preferred_element_type=jnp.float32) * scale
        positive = lax.optimization_barrier(jnp.sum(rows.astype(jnp.float32) * pos_rows.astype(jnp.float32), axis=1)) * scale
        hit = row_ids[:, None] == negative_ids[None, :]
        masked = jnp.where(hit, -jnp.inf, logits)
        peak = jnp.maximum(lax.optimization_barrier(jnp.max(masked, axis=1)), positive)
        summed = lax.optimization_barrier(jnp.sum(jnp.exp(masked - peak[:, None]), axis=1)) + jnp.exp(positive - peak)
        return peak + jnp.log(summed) - positive
    losses = lax.map(one_block, (users_blocks, pos_blocks, ids_blocks)).reshape(TOKENS)
    group_size = TOKENS // N_DP
    positions = jnp.arange(group_size, dtype=jnp.int32)
    ends = offsets[:, 1:]
    last_slot = jnp.any(positions[None, :, None] + 1 == ends[:, None, :], axis=2)
    live = (positions[None, :] < offsets[:, USERS:USERS + 1]) & jnp.logical_not(last_slot)
    live = live.reshape(TOKENS)
    token_loss = jnp.where(live, losses, jnp.float32(0.0)).astype(jnp.float32)
    weight = token_weights.astype(jnp.float32)
    total = jnp.sum(weight * token_loss)
    count = jnp.sum(weight * live.astype(jnp.float32))
    return (token_loss, total / count)
```

```python
import functools
import math

import jax
import jax.numpy as jnp
from jax import lax
from jax.experimental import pallas as pl
from jax.experimental.pallas import tpu as pltpu
from jax.sharding import PartitionSpec as P

MESH = pl.DeviceIdType.MESH
LOG2E = math.log2(math.e)
LN2 = math.log(2.0)
MASKED = -1e30
FLOOR = -1e20
NEG = 4
TILES = 3
STEPS = NEG * TILES
FROM_LEFT = {0: 3, 1: 5, 2: 7}
FROM_RIGHT = {2: 4, 1: 6, 0: 8}
FROM_FAR = {0: 9, 2: 10, 1: 11}


def nt_dot(a, b):
    return lax.dot_general(a, b, (((1,), (1,)), ((), ())), preferred_element_type=jnp.float32)


def kernel(
    dims, chunk, scale2,
    user, positive, row_ids, weights, offsets, neg, neg_ids,
    loss_out, mean_out,
    rows_v, ids_v, pos_v, neg_v, nid_v, bufs, part, got, sum_a, sum_b,
    load_sem, row_send, fwd_send, row_recv, id_send, id_recv, part_send, part_recv,
    a_send, a_recv, b_send, b_recv,
):
    ny, nz, nc = dims
    per_y = nz * nc
    n = lax.axis_index("neg")
    d = lax.axis_index("dp")
    y, inner = d // per_y, d % per_y
    z, core = inner // nc, inner % nc
    right, left, far = (n + 1) % NEG, (n + 3) % NEG, (n + 2) % NEG
    tile = rows_v.shape[0] // STEPS
    half = tile // 2
    halves = tile // 128
    tokens = TILES * tile
    negs = neg_v.shape[0]
    number = negs // chunk
    group = chunk // 8

    peers_a = [
        (k, ((y + k // NEG) % ny) * per_y + inner, (n + k % NEG) % NEG) for k in range(1, ny * NEG)
    ]
    peers_b = [
        (k, y * per_y + ((z + k // nc) % nz) * nc + (core + k % nc) % nc, n)
        for k in range(1, per_y)
    ]

    own = rows_v.at[pl.ds(0, tokens), :]
    loads = [
        pltpu.make_async_copy(user, own, load_sem.at[0]),
        pltpu.make_async_copy(row_ids, ids_v.at[pl.ds(0, TILES)], load_sem.at[1]),
        pltpu.make_async_copy(neg, neg_v, load_sem.at[2]),
        pltpu.make_async_copy(positive, pos_v, load_sem.at[3]),
    ]
    for load in loads:
        load.start()

    barrier = pltpu.get_barrier_semaphore()
    for _, dp_to, neg_to in peers_a + peers_b:
        pl.semaphore_signal(barrier, inc=1, device_id=(dp_to, neg_to), device_id_type=MESH)

    for r in range(negs // 128):
        nid_v[r * 128 : (r + 1) * 128, :] = jnp.broadcast_to(
            neg_ids[r : r + 1, :], (128, 128)
        ).T
    for load in loads[:2]:
        load.wait()
    pl.semaphore_wait(barrier, len(peers_a) + len(peers_b))

    def rows_at(step, start=0, size=None):
        return rows_v.at[pl.ds(step * tile + start, size or tile), :]

    def remote(src, dst, send, recv, to):
        return pltpu.make_async_remote_copy(
            src_ref=src, dst_ref=dst, send_sem=send, recv_sem=recv,
            device_id=(d, to), device_id_type=MESH,
        )

    def id_copy(index, j, step, to):
        return remote(ids_v.at[j], ids_v.at[step], id_send.at[index], id_recv.at[step], to)

    def row_copy(index, j, step, to):
        return remote(rows_at(j), rows_at(step), row_send.at[index], row_recv.at[step], to)

    id_copies, row_copies = [], []
    for j in range(TILES):
        for table, to in ((FROM_LEFT, right), (FROM_RIGHT, left), (FROM_FAR, far)):
            id_copies.append(id_copy(len(id_copies), j, table[j], to))
    for jr, jl in ((0, 2), (1, 1), (2, 0)):
        row_copies.append(row_copy(len(row_copies), jr, FROM_LEFT[jr], right))
        row_copies.append(row_copy(len(row_copies), jl, FROM_RIGHT[jl], left))
    for copy in id_copies + row_copies:
        copy.start()

    forward = [
        remote(rows_at(3), rows_at(9), fwd_send.at[0], row_recv.at[9], right),
        remote(rows_at(4), rows_at(10), fwd_send.at[1], row_recv.at[10], left),
        remote(rows_at(5, 0, half), rows_at(11, 0, half), fwd_send.at[2], row_recv.at[11], right),
        remote(
            rows_at(6, half, half), rows_at(11, half, half), fwd_send.at[3], row_recv.at[12], left
        ),
    ]
    loads[2].wait()

    def one_tile(s, carry):
        @pl.when(jnp.logical_and(s >= 3, s < 11))
        def _():
            remote(rows_at(0), rows_at(s), row_send.at[0], row_recv.at[s], right).wait_recv()

        @pl.when(s >= 3)
        def _():
            remote(ids_v.at[0], ids_v.at[s], id_send.at[0], id_recv.at[s], right).wait_recv()

        @pl.when(s == 11)
        def _():
            forward[2].wait_recv()
            forward[3].wait_recv()

        @pl.when(s == 4)
        def _():
            forward[0].start()
            forward[1].start()

        @pl.when(s == 6)
        def _():
            forward[2].start()
            forward[3].start()

        u = rows_v.at[pl.ds(pl.multiple_of(s * tile, tile), tile), :]
        rid = [ids_v[s, :, h * 128 : (h + 1) * 128] for h in range(halves)]

        def front(c):
            logits = nt_dot(neg_v[c * chunk : (c + 1) * chunk, :], u[...])
            peaks = []
            for h in range(halves):
                x = logits[:, h * 128 : (h + 1) * 128] * scale2
                x = jnp.where(nid_v[c * chunk : (c + 1) * chunk, :] == rid[h], MASKED, x)
                bufs[c % 2, :, h * 128 : (h + 1) * 128] = x
                peaks.append(jnp.max(x.reshape(group, 8, 128), axis=0))
            return peaks

        def back(state, peaks, c):
            out = []
            for h in range(halves):
                peak, total = state[h]
                new = jnp.maximum(peak, peaks[h])
                x = bufs[c % 2, :, h * 128 : (h + 1) * 128].reshape(group // 4, 4, 8, 128)
                e = jnp.sum(jnp.exp2(x - new[None, None]), axis=0)
                out.append((new, total * jnp.exp2(peak - new) + jnp.sum(e, axis=0)))
            return out

        state = [
            (jnp.full((8, 128), FLOOR, jnp.float32), jnp.zeros((8, 128), jnp.float32))
            for _ in range(halves)
        ]
        peaks = front(0)
        for c in range(number):
            later = front(c + 1) if c + 1 < number else None
            state = back(state, peaks, c)
            peaks = later
        for h, (peak, total) in enumerate(state):
            top = jnp.max(peak, axis=0, keepdims=True)
            total = jnp.sum(total * jnp.exp2(peak - top), axis=0, keepdims=True)
            value = jnp.where(total > 0.0, top + jnp.log2(jnp.maximum(total, 1e-37)), MASKED)
            part[s, :, h * 128 : (h + 1) * 128] = value
        return carry

    lax.fori_loop(0, STEPS, one_tile, 0)

    part_copies = []
    for slot, table, to in ((3, FROM_FAR, far), (1, FROM_LEFT, left), (2, FROM_RIGHT, right)):
        for j in range(TILES):
            index = len(part_copies)
            part_copies.append(
                remote(part.at[table[j]], got.at[slot, j], part_send.at[index],
                       part_recv.at[index], to)
            )
    for copy in part_copies:
        copy.start()

    loads[3].wait()
    ones = jnp.ones((8, rows_v.shape[1]), jnp.bfloat16)
    lane = lax.broadcasted_iota(jnp.int32, (1, tile), 1)
    ready = []
    for j in range(TILES):
        product = rows_v[j * tile : (j + 1) * tile, :].astype(jnp.float32) * pos_v[
            j * tile : (j + 1) * tile, :
        ].astype(jnp.float32)
        high = product.astype(jnp.bfloat16)
        low = (product - high.astype(jnp.float32)).astype(jnp.bfloat16)
        pos2 = (nt_dot(ones, high) + nt_dot(ones, low))[0:1, :] * scale2
        place = n * tokens + j * tile + lane
        live = place < offsets[0, offsets.shape[1] - 1]
        for k in range(1, offsets.shape[1]):
            live = jnp.logical_and(live, place + 1 != offsets[0, k])
        ready.append((pos2, live, weights[j].astype(jnp.float32)))

    for copy in part_copies:
        copy.wait_recv()
    total = jnp.zeros((1, 128), jnp.float32)
    count = jnp.zeros((1, 128), jnp.float32)
    for j, (pos2, live, weight) in enumerate(ready):
        terms = [pos2, part[j], got[1, j], got[2, j], got[3, j]]
        top = functools.reduce(jnp.maximum, terms)
        summed = functools.reduce(jnp.add, [jnp.exp2(term - top) for term in terms])
        loss = jnp.where(live, (top - pos2 + jnp.log2(summed)) * LN2, 0.0)
        loss_out[j] = loss
        weighted = weight * loss
        counted = jnp.where(live, weight, 0.0)
        for h in range(halves):
            total = total + weighted[:, h * 128 : (h + 1) * 128]
            count = count + counted[:, h * 128 : (h + 1) * 128]

    def exchange(buffer, mine, peers, send, recv):
        copies = [
            pltpu.make_async_remote_copy(
                src_ref=buffer.at[mine], dst_ref=buffer.at[mine], send_sem=send.at[k],
                recv_sem=recv.at[k], device_id=(dp_to, neg_to), device_id_type=MESH,
            )
            for k, dp_to, neg_to in peers
        ]
        for copy in copies:
            copy.start()
        return copies

    def summed_slots(buffer):
        parts = [buffer[k] for k in range(buffer.shape[0])]
        while len(parts) > 1:
            parts = [a + b for a, b in zip(parts[::2], parts[1::2])]
        return parts[0]

    slot_a = y * NEG + n
    sum_a[slot_a, 0:1, :] = total
    sum_a[slot_a, 1:2, :] = count
    copies_a = exchange(sum_a, slot_a, peers_a, a_send, a_recv)
    for copy in copies_a:
        copy.wait_recv()
    sum_b[inner] = summed_slots(sum_a)
    copies_b = exchange(sum_b, inner, peers_b, b_send, b_recv)
    for copy in row_copies + id_copies + forward + part_copies + copies_a:
        copy.wait_send()
    for copy in copies_b:
        copy.wait_recv()
    both = summed_slots(sum_b)
    mean_out[...] = jnp.sum(both[0:1, :], axis=1, keepdims=True) / jnp.sum(
        both[1:2, :], axis=1, keepdims=True
    )
    for copy in copies_b:
        copy.wait_send()


def build(dims, chunk):
    def shards(user, positive, row_ids, weights, offsets, neg, neg_ids):
        tokens, width = user.shape
        negs = neg.shape[0]
        tile = tokens // TILES
        ny, nz, nc = dims
        size_a, size_b = ny * NEG, nz * nc
        in_any = pl.BlockSpec(memory_space=pl.ANY)
        in_vmem = pl.BlockSpec(memory_space=pltpu.VMEM)
        dma = pltpu.SemaphoreType.DMA
        f32, bf16, i32 = jnp.float32, jnp.bfloat16, jnp.int32
        flops = 2 * NEG * tokens * negs * width
        loss, mean = pl.pallas_call(
            functools.partial(kernel, dims, chunk, 3.0 / math.sqrt(width) * LOG2E),
            out_shape=(
                jax.ShapeDtypeStruct((TILES, 1, tile), f32),
                jax.ShapeDtypeStruct((1, 1), f32),
            ),
            in_specs=[
                in_any, in_any, in_vmem, in_vmem, pl.BlockSpec(memory_space=pltpu.SMEM),
                in_any, in_vmem,
            ],
            out_specs=(in_vmem, in_vmem),
            scratch_shapes=[
                pltpu.VMEM((STEPS * tile, width), bf16),
                pltpu.VMEM((STEPS, 1, tile), i32),
                pltpu.VMEM((tokens, width), bf16),
                pltpu.VMEM((negs, width), bf16),
                pltpu.VMEM((negs, 128), i32),
                pltpu.VMEM((2, chunk, tile), f32),
                pltpu.VMEM((STEPS, 1, tile), f32),
                pltpu.VMEM((NEG, TILES, 1, tile), f32),
                pltpu.VMEM((size_a, 2, 128), f32),
                pltpu.VMEM((size_b, 2, 128), f32),
                dma((4,)), dma((6,)), dma((4,)), dma((13,)), dma((9,)), dma((12,)),
                dma((9,)), dma((9,)),
                dma((size_a,)), dma((size_a,)), dma((size_b,)), dma((size_b,)),
            ],
            compiler_params=pltpu.CompilerParams(
                collective_id=0, has_side_effects=True, vmem_limit_bytes=48 * 2**20
            ),
            cost_estimate=pl.CostEstimate(
                flops=flops, bytes_accessed=2 * negs * width, transcendentals=0
            ),
        )(
            user, positive, row_ids.reshape(TILES, 1, tile), weights.reshape(TILES, 1, tile),
            offsets, neg, neg_ids.reshape(negs // 128, 128),
        )
        return loss.reshape(tokens), mean.reshape(())

    return shards


def on_mesh(mesh, dims, chunk):
    both = ("dp", "neg")
    return jax.shard_map(
        build(dims, chunk),
        mesh=mesh,
        in_specs=(
            P(both, None), P(both, None), P(both), P(both), P("dp", None),
            P("neg", None), P("neg"),
        ),
        out_specs=(P(both), P()),
        check_vma=False,
    )


def solution(mesh):
    return on_mesh(mesh, (4, 8, 2), 512)
```

```python
import functools
import math

import jax
import jax.numpy as jnp
from jax import lax
from jax.experimental import pallas as pl
from jax.experimental.pallas import tpu as pltpu
from jax.sharding import PartitionSpec as P

MESH = pl.DeviceIdType.MESH
LOG2E = math.log2(math.e)
LN2 = math.log(2.0)
MASKED = -1e30
FLOOR = -1e20
NEG = 4
TILES = 3
STEPS = NEG * TILES
FROM_LEFT = {0: 3, 1: 5, 2: 7}
FROM_RIGHT = {2: 4, 1: 6, 0: 8}
FROM_FAR = {0: 9, 2: 10, 1: 11}


def nt_dot(a, b):
    return lax.dot_general(a, b, (((1,), (1,)), ((), ())), preferred_element_type=jnp.float32)


def kernel(
    dims, chunk, scale2,
    user, positive, row_ids, weights, offsets, neg, neg_ids,
    loss_out, mean_out,
    rows_v, ids_v, pos_v, neg_v, nid_v, bufs, part, got, sum_a, sum_b,
    id_rows, weight_rows, nid_rows, ends,
    load_sem, row_send, fwd_send, row_recv, id_send, id_recv, part_send, part_recv,
    a_send, a_recv, b_send, b_recv,
):
    ny, nz, nc = dims
    per_y = nz * nc
    n = lax.axis_index("neg")
    d = lax.axis_index("dp")
    y, inner = d // per_y, d % per_y
    z, core = inner // nc, inner % nc
    right, left, far = (n + 1) % NEG, (n + 3) % NEG, (n + 2) % NEG
    tile = rows_v.shape[0] // STEPS
    half = tile // 2
    halves = tile // 128
    tokens = TILES * tile
    negs = neg_v.shape[0]
    number = negs // chunk
    group = chunk // 8

    peers_a = [
        (k, ((y + k // NEG) % ny) * per_y + inner, (n + k % NEG) % NEG) for k in range(1, ny * NEG)
    ]
    peers_b = [
        (k, y * per_y + ((z + k // nc) % nz) * nc + (core + k % nc) % nc, n)
        for k in range(1, per_y)
    ]

    own = rows_v.at[pl.ds(0, tokens), :]
    pairs = (
        (neg_ids, nid_rows), (row_ids, id_rows), (user, own), (neg, neg_v),
        (positive, pos_v), (weights, weight_rows), (offsets, ends),
    )
    loads = [
        pltpu.make_async_copy(src, dst, load_sem.at[k]) for k, (src, dst) in enumerate(pairs)
    ]
    for load in loads:
        load.start()

    barrier = pltpu.get_barrier_semaphore()
    for _, dp_to, neg_to in peers_a + peers_b:
        pl.semaphore_signal(barrier, inc=1, device_id=(dp_to, neg_to), device_id_type=MESH)

    loads[0].wait()
    loads[1].wait()
    for j in range(TILES):
        for h in range(halves):
            row = j * halves + h
            ids_v[j, :, h * 128 : (h + 1) * 128] = id_rows[row : row + 1, :]
    for r in range(negs // 128):
        nid_v[r * 128 : (r + 1) * 128, :] = jnp.broadcast_to(
            nid_rows[r : r + 1, :], (128, 128)
        ).T
    loads[2].wait()
    pl.semaphore_wait(barrier, len(peers_a) + len(peers_b))

    def rows_at(step, start=0, size=None):
        return rows_v.at[pl.ds(step * tile + start, size or tile), :]

    def remote(src, dst, send, recv, to):
        return pltpu.make_async_remote_copy(
            src_ref=src, dst_ref=dst, send_sem=send, recv_sem=recv,
            device_id=(d, to), device_id_type=MESH,
        )

    def id_copy(index, j, step, to):
        return remote(ids_v.at[j], ids_v.at[step], id_send.at[index], id_recv.at[step], to)

    def row_copy(index, j, step, to):
        return remote(rows_at(j), rows_at(step), row_send.at[index], row_recv.at[step], to)

    id_copies, row_copies = [], []
    for j in range(TILES):
        for table, to in ((FROM_LEFT, right), (FROM_RIGHT, left), (FROM_FAR, far)):
            id_copies.append(id_copy(len(id_copies), j, table[j], to))
    for jr, jl in ((0, 2), (1, 1), (2, 0)):
        row_copies.append(row_copy(len(row_copies), jr, FROM_LEFT[jr], right))
        row_copies.append(row_copy(len(row_copies), jl, FROM_RIGHT[jl], left))
    for copy in id_copies + row_copies:
        copy.start()

    forward = [
        remote(rows_at(3), rows_at(9), fwd_send.at[0], row_recv.at[9], right),
        remote(rows_at(4), rows_at(10), fwd_send.at[1], row_recv.at[10], left),
        remote(rows_at(5, 0, half), rows_at(11, 0, half), fwd_send.at[2], row_recv.at[11], right),
        remote(
            rows_at(6, half, half), rows_at(11, half, half), fwd_send.at[3], row_recv.at[12], left
        ),
    ]
    loads[3].wait()

    def one_tile(s, carry):
        @pl.when(jnp.logical_and(s >= 3, s < 11))
        def _():
            remote(rows_at(0), rows_at(s), row_send.at[0], row_recv.at[s], right).wait_recv()

        @pl.when(s >= 3)
        def _():
            remote(ids_v.at[0], ids_v.at[s], id_send.at[0], id_recv.at[s], right).wait_recv()

        @pl.when(s == 11)
        def _():
            forward[2].wait_recv()
            forward[3].wait_recv()

        @pl.when(s == 4)
        def _():
            forward[0].start()
            forward[1].start()

        @pl.when(s == 6)
        def _():
            forward[2].start()
            forward[3].start()

        u = rows_v.at[pl.ds(pl.multiple_of(s * tile, tile), tile), :]
        rid = [ids_v[s, :, h * 128 : (h + 1) * 128] for h in range(halves)]

        def front(c):
            logits = nt_dot(neg_v[c * chunk : (c + 1) * chunk, :], u[...])
            peaks = []
            for h in range(halves):
                x = logits[:, h * 128 : (h + 1) * 128] * scale2
                x = jnp.where(nid_v[c * chunk : (c + 1) * chunk, :] == rid[h], MASKED, x)
                bufs[c % 2, :, h * 128 : (h + 1) * 128] = x
                peaks.append(jnp.max(x.reshape(group, 8, 128), axis=0))
            return peaks

        def back(state, peaks, c):
            out = []
            for h in range(halves):
                peak, total = state[h]
                new = jnp.maximum(peak, peaks[h])
                x = bufs[c % 2, :, h * 128 : (h + 1) * 128].reshape(group // 4, 4, 8, 128)
                e = jnp.sum(jnp.exp2(x - new[None, None]), axis=0)
                out.append((new, total * jnp.exp2(peak - new) + jnp.sum(e, axis=0)))
            return out

        state = [
            (jnp.full((8, 128), FLOOR, jnp.float32), jnp.zeros((8, 128), jnp.float32))
            for _ in range(halves)
        ]
        peaks = front(0)
        for c in range(number):
            later = front(c + 1) if c + 1 < number else None
            state = back(state, peaks, c)
            peaks = later
        for h, (peak, total) in enumerate(state):
            top = jnp.max(peak, axis=0, keepdims=True)
            total = jnp.sum(total * jnp.exp2(peak - top), axis=0, keepdims=True)
            value = jnp.where(total > 0.0, top + jnp.log2(jnp.maximum(total, 1e-37)), MASKED)
            part[s, :, h * 128 : (h + 1) * 128] = value
        return carry

    lax.fori_loop(0, STEPS, one_tile, 0)

    part_copies = []
    for slot, table, to in ((3, FROM_FAR, far), (1, FROM_LEFT, left), (2, FROM_RIGHT, right)):
        for j in range(TILES):
            index = len(part_copies)
            part_copies.append(
                remote(part.at[table[j]], got.at[slot, j], part_send.at[index],
                       part_recv.at[index], to)
            )
    for copy in part_copies:
        copy.start()

    for load in loads[4:]:
        load.wait()
    ones = jnp.ones((8, rows_v.shape[1]), jnp.bfloat16)
    lane = lax.broadcasted_iota(jnp.int32, (1, tile), 1)
    ready = []
    for j in range(TILES):
        product = rows_v[j * tile : (j + 1) * tile, :].astype(jnp.float32) * pos_v[
            j * tile : (j + 1) * tile, :
        ].astype(jnp.float32)
        high = product.astype(jnp.bfloat16)
        low = (product - high.astype(jnp.float32)).astype(jnp.bfloat16)
        pos2 = (nt_dot(ones, high) + nt_dot(ones, low))[0:1, :] * scale2
        place = n * tokens + j * tile + lane
        live = place < ends[0, ends.shape[1] - 1]
        for k in range(1, ends.shape[1]):
            live = jnp.logical_and(live, place + 1 != ends[0, k])
        ready.append((pos2, live))

    for copy in part_copies:
        copy.wait_recv()
    total = jnp.zeros((1, 128), jnp.float32)
    count = jnp.zeros((1, 128), jnp.float32)
    for j, (pos2, live) in enumerate(ready):
        terms = [pos2, part[j], got[1, j], got[2, j], got[3, j]]
        top = functools.reduce(jnp.maximum, terms)
        summed = functools.reduce(jnp.add, [jnp.exp2(term - top) for term in terms])
        loss = jnp.where(live, (top - pos2 + jnp.log2(summed)) * LN2, 0.0)
        alive = jnp.where(live, 1.0, 0.0)
        for h in range(halves):
            row = j * halves + h
            weight = weight_rows[row : row + 1, :].astype(jnp.float32)
            loss_out[row : row + 1, :] = loss[:, h * 128 : (h + 1) * 128]
            total = total + weight * loss[:, h * 128 : (h + 1) * 128]
            count = count + weight * alive[:, h * 128 : (h + 1) * 128]

    def exchange(buffer, mine, peers, send, recv):
        copies = [
            pltpu.make_async_remote_copy(
                src_ref=buffer.at[mine], dst_ref=buffer.at[mine], send_sem=send.at[k],
                recv_sem=recv.at[k], device_id=(dp_to, neg_to), device_id_type=MESH,
            )
            for k, dp_to, neg_to in peers
        ]
        for copy in copies:
            copy.start()
        return copies

    def summed_slots(buffer):
        parts = [buffer[k] for k in range(buffer.shape[0])]
        while len(parts) > 1:
            parts = [a + b for a, b in zip(parts[::2], parts[1::2])]
        return parts[0]

    slot_a = y * NEG + n
    sum_a[slot_a, 0:1, :] = total
    sum_a[slot_a, 1:2, :] = count
    copies_a = exchange(sum_a, slot_a, peers_a, a_send, a_recv)
    for copy in copies_a:
        copy.wait_recv()
    sum_b[inner] = summed_slots(sum_a)
    copies_b = exchange(sum_b, inner, peers_b, b_send, b_recv)
    for copy in row_copies + id_copies + forward + part_copies + copies_a:
        copy.wait_send()
    for copy in copies_b:
        copy.wait_recv()
    both = summed_slots(sum_b)
    mean_out[...] = jnp.sum(both[0:1, :], axis=1, keepdims=True) / jnp.sum(
        both[1:2, :], axis=1, keepdims=True
    )
    for copy in copies_b:
        copy.wait_send()


def build(dims, chunk):
    def shards(user, positive, row_ids, weights, offsets, neg, neg_ids):
        tokens, width = user.shape
        negs = neg.shape[0]
        tile, lines = tokens // TILES, tokens // 128
        ny, nz, nc = dims
        size_a, size_b = ny * NEG, nz * nc
        in_any = pl.BlockSpec(memory_space=pl.ANY)
        in_vmem = pl.BlockSpec(memory_space=pltpu.VMEM)
        dma = pltpu.SemaphoreType.DMA
        f32, bf16, i32 = jnp.float32, jnp.bfloat16, jnp.int32
        flops = 2 * NEG * tokens * negs * width
        loss, mean = pl.pallas_call(
            functools.partial(kernel, dims, chunk, 3.0 / math.sqrt(width) * LOG2E),
            out_shape=(
                jax.ShapeDtypeStruct((lines, 128), f32),
                jax.ShapeDtypeStruct((1, 1), f32),
            ),
            in_specs=[in_any] * 7,
            out_specs=(in_vmem, in_vmem),
            scratch_shapes=[
                pltpu.VMEM((STEPS * tile, width), bf16),
                pltpu.VMEM((STEPS, 1, tile), i32),
                pltpu.VMEM((tokens, width), bf16),
                pltpu.VMEM((negs, width), bf16),
                pltpu.VMEM((negs, 128), i32),
                pltpu.VMEM((2, chunk, tile), f32),
                pltpu.VMEM((STEPS, 1, tile), f32),
                pltpu.VMEM((NEG, TILES, 1, tile), f32),
                pltpu.VMEM((size_a, 2, 128), f32),
                pltpu.VMEM((size_b, 2, 128), f32),
                pltpu.VMEM((lines, 128), i32),
                pltpu.VMEM((lines, 128), i32),
                pltpu.VMEM((negs // 128, 128), i32),
                pltpu.SMEM(offsets.shape, i32),
                dma((7,)), dma((6,)), dma((4,)), dma((13,)), dma((9,)), dma((12,)),
                dma((9,)), dma((9,)),
                dma((size_a,)), dma((size_a,)), dma((size_b,)), dma((size_b,)),
            ],
            compiler_params=pltpu.CompilerParams(
                collective_id=0, has_side_effects=True
            ),
            cost_estimate=pl.CostEstimate(
                flops=flops, bytes_accessed=2 * negs * width, transcendentals=0
            ),
        )(
            user, positive, row_ids.reshape(lines, 128), weights.reshape(lines, 128),
            offsets, neg, neg_ids.reshape(negs // 128, 128),
        )
        return loss.reshape(tokens), mean.reshape(())

    return shards


def on_mesh(mesh, dims, chunk):
    both = ("dp", "neg")
    return jax.shard_map(
        build(dims, chunk),
        mesh=mesh,
        in_specs=(
            P(both, None), P(both, None), P(both), P(both), P("dp", None),
            P("neg", None), P("neg"),
        ),
        out_specs=(P(both), P()),
        check_vma=False,
    )


def solution(mesh):
    return on_mesh(mesh, (4, 8, 2), 256)
```

```python
import functools
import math

import jax
import jax.numpy as jnp
from jax import lax
from jax.experimental import pallas as pl
from jax.experimental.pallas import tpu as pltpu
from jax.sharding import PartitionSpec as P

MESH = pl.DeviceIdType.MESH
LOG2E = math.log2(math.e)
LN2 = math.log(2.0)
MASKED = -1e30
FLOOR = -1e20
NEG = 4
TILES = 3
STEPS = NEG * TILES
BLOCK = 128
FROM_LEFT = {0: 3, 1: 5, 2: 7}
FROM_RIGHT = {2: 4, 1: 6, 0: 8}
FROM_FAR = {0: 9, 2: 10, 1: 11}


def nt_dot(a, b):
    return lax.dot_general(a, b, (((1,), (1,)), ((), ())), preferred_element_type=jnp.float32)


def kernel(
    dims, chunk, scale2,
    user, positive, row_ids, weights, offsets, neg, neg_ids,
    loss_out, mean_out,
    rows_v, ids_v, pos_v, neg_v, nid_v, part, got, sum_a, sum_b,
    id_rows, weight_rows, nid_rows, ends,
    load_sem, row_send, fwd_send, row_recv, id_send, id_recv, part_send, part_recv,
    a_send, a_recv, b_send, b_recv,
):
    ny, nz, nc = dims
    per_y = nz * nc
    n = lax.axis_index("neg")
    d = lax.axis_index("dp")
    y, inner = d // per_y, d % per_y
    z, core = inner // nc, inner % nc
    right, left, far = (n + 1) % NEG, (n + 3) % NEG, (n + 2) % NEG
    tile = rows_v.shape[0] // STEPS
    half = tile // 2
    halves = tile // 128
    tokens = TILES * tile
    negs = neg_v.shape[0]

    peers_a = [
        (k, ((y + k // NEG) % ny) * per_y + inner, (n + k % NEG) % NEG) for k in range(1, ny * NEG)
    ]
    peers_b = [
        (k, y * per_y + ((z + k // nc) % nz) * nc + (core + k % nc) % nc, n)
        for k in range(1, per_y)
    ]

    own = rows_v.at[pl.ds(0, tokens), :]
    pairs = (
        (neg_ids, nid_rows), (row_ids, id_rows), (user, own), (neg, neg_v),
        (positive, pos_v), (weights, weight_rows), (offsets, ends),
    )
    loads = [
        pltpu.make_async_copy(src, dst, load_sem.at[k]) for k, (src, dst) in enumerate(pairs)
    ]
    for load in loads:
        load.start()

    barrier = pltpu.get_barrier_semaphore()
    for _, dp_to, neg_to in peers_a + peers_b:
        pl.semaphore_signal(barrier, inc=1, device_id=(dp_to, neg_to), device_id_type=MESH)

    loads[0].wait()
    loads[1].wait()
    for j in range(TILES):
        for h in range(halves):
            row = j * halves + h
            ids_v[j, :, h * 128 : (h + 1) * 128] = id_rows[row : row + 1, :]
    for r in range(negs // 128):
        nid_v[r * 128 : (r + 1) * 128, :] = jnp.broadcast_to(
            nid_rows[r : r + 1, :], (128, 128)
        ).T
    loads[2].wait()
    pl.semaphore_wait(barrier, len(peers_a) + len(peers_b))

    def rows_at(step, start=0, size=None):
        return rows_v.at[pl.ds(step * tile + start, size or tile), :]

    def remote(src, dst, send, recv, to):
        return pltpu.make_async_remote_copy(
            src_ref=src, dst_ref=dst, send_sem=send, recv_sem=recv,
            device_id=(d, to), device_id_type=MESH,
        )

    def id_copy(index, j, step, to):
        return remote(ids_v.at[j], ids_v.at[step], id_send.at[index], id_recv.at[step], to)

    def row_copy(index, j, step, to):
        return remote(rows_at(j), rows_at(step), row_send.at[index], row_recv.at[step], to)

    id_copies, row_copies = [], []
    for j in range(TILES):
        for table, to in ((FROM_LEFT, right), (FROM_RIGHT, left), (FROM_FAR, far)):
            id_copies.append(id_copy(len(id_copies), j, table[j], to))
    for jr, jl in ((0, 2), (1, 1), (2, 0)):
        row_copies.append(row_copy(len(row_copies), jr, FROM_LEFT[jr], right))
        row_copies.append(row_copy(len(row_copies), jl, FROM_RIGHT[jl], left))
    for copy in id_copies + row_copies:
        copy.start()

    forward = [
        remote(rows_at(3), rows_at(9), fwd_send.at[0], row_recv.at[9], right),
        remote(rows_at(4), rows_at(10), fwd_send.at[1], row_recv.at[10], left),
        remote(rows_at(5, 0, half), rows_at(11, 0, half), fwd_send.at[2], row_recv.at[11], right),
        remote(
            rows_at(6, half, half), rows_at(11, half, half), fwd_send.at[3], row_recv.at[12], left
        ),
    ]
    loads[3].wait()

    def one_tile(s, carry):
        @pl.when(jnp.logical_and(s >= 3, s < 11))
        def _():
            remote(rows_at(0), rows_at(s), row_send.at[0], row_recv.at[s], right).wait_recv()

        @pl.when(s >= 3)
        def _():
            remote(ids_v.at[0], ids_v.at[s], id_send.at[0], id_recv.at[s], right).wait_recv()

        @pl.when(s == 11)
        def _():
            forward[2].wait_recv()
            forward[3].wait_recv()

        @pl.when(s == 4)
        def _():
            forward[0].start()
            forward[1].start()

        @pl.when(s == 6)
        def _():
            forward[2].start()
            forward[3].start()

        u = rows_v.at[pl.ds(pl.multiple_of(s * tile, tile), tile), :]
        rid = [ids_v[s, :, h * 128 : (h + 1) * 128] for h in range(halves)]

        state = [
            (jnp.full((8, 128), FLOOR, jnp.float32), jnp.zeros((8, 128), jnp.float32))
            for _ in range(halves)
        ]
        for c in range(negs // chunk):
            logits = nt_dot(neg_v[c * chunk : (c + 1) * chunk, :], u[...])
            for b in range(0, chunk, BLOCK):
                at = c * chunk + b
                for h in range(halves):
                    x = logits[b : b + BLOCK, h * 128 : (h + 1) * 128] * scale2
                    x = jnp.where(nid_v[at : at + BLOCK, :] == rid[h], MASKED, x)
                    x = x.reshape(BLOCK // 8, 8, 128)
                    peak, total = state[h]
                    new = jnp.maximum(peak, jnp.max(x, axis=0))
                    e = jnp.sum(jnp.exp2(x - new[None]), axis=0)
                    state[h] = (new, total * jnp.exp2(peak - new) + e)
        for h, (peak, total) in enumerate(state):
            top = jnp.max(peak, axis=0, keepdims=True)
            total = jnp.sum(total * jnp.exp2(peak - top), axis=0, keepdims=True)
            value = jnp.where(total > 0.0, top + jnp.log2(jnp.maximum(total, 1e-37)), MASKED)
            part[s, :, h * 128 : (h + 1) * 128] = value
        return carry

    lax.fori_loop(0, STEPS, one_tile, 0)

    part_copies = []
    for slot, table, to in ((3, FROM_FAR, far), (1, FROM_LEFT, left), (2, FROM_RIGHT, right)):
        for j in range(TILES):
            index = len(part_copies)
            part_copies.append(
                remote(part.at[table[j]], got.at[slot, j], part_send.at[index],
                       part_recv.at[index], to)
            )
    for copy in part_copies:
        copy.start()

    for load in loads[4:]:
        load.wait()
    ones = jnp.ones((8, rows_v.shape[1]), jnp.bfloat16)
    lane = lax.broadcasted_iota(jnp.int32, (1, tile), 1)
    ready = []
    for j in range(TILES):
        product = rows_v[j * tile : (j + 1) * tile, :].astype(jnp.float32) * pos_v[
            j * tile : (j + 1) * tile, :
        ].astype(jnp.float32)
        high = product.astype(jnp.bfloat16)
        low = (product - high.astype(jnp.float32)).astype(jnp.bfloat16)
        pos2 = (nt_dot(ones, high) + nt_dot(ones, low))[0:1, :] * scale2
        place = n * tokens + j * tile + lane
        live = place < ends[0, ends.shape[1] - 1]
        for k in range(1, ends.shape[1]):
            live = jnp.logical_and(live, place + 1 != ends[0, k])
        ready.append((pos2, live))

    for copy in part_copies:
        copy.wait_recv()
    total = jnp.zeros((1, 128), jnp.float32)
    count = jnp.zeros((1, 128), jnp.float32)
    for j, (pos2, live) in enumerate(ready):
        terms = [pos2, part[j], got[1, j], got[2, j], got[3, j]]
        top = functools.reduce(jnp.maximum, terms)
        summed = functools.reduce(jnp.add, [jnp.exp2(term - top) for term in terms])
        loss = jnp.where(live, (top - pos2 + jnp.log2(summed)) * LN2, 0.0)
        alive = jnp.where(live, 1.0, 0.0)
        for h in range(halves):
            row = j * halves + h
            weight = weight_rows[row : row + 1, :].astype(jnp.float32)
            loss_out[row : row + 1, :] = loss[:, h * 128 : (h + 1) * 128]
            total = total + weight * loss[:, h * 128 : (h + 1) * 128]
            count = count + weight * alive[:, h * 128 : (h + 1) * 128]

    def exchange(buffer, mine, peers, send, recv):
        copies = [
            pltpu.make_async_remote_copy(
                src_ref=buffer.at[mine], dst_ref=buffer.at[mine], send_sem=send.at[k],
                recv_sem=recv.at[k], device_id=(dp_to, neg_to), device_id_type=MESH,
            )
            for k, dp_to, neg_to in peers
        ]
        for copy in copies:
            copy.start()
        return copies

    def summed_slots(buffer):
        parts = [buffer[k] for k in range(buffer.shape[0])]
        while len(parts) > 1:
            parts = [a + b for a, b in zip(parts[::2], parts[1::2])]
        return parts[0]

    slot_a = y * NEG + n
    sum_a[slot_a, 0:1, :] = total
    sum_a[slot_a, 1:2, :] = count
    copies_a = exchange(sum_a, slot_a, peers_a, a_send, a_recv)
    for copy in copies_a:
        copy.wait_recv()
    sum_b[inner] = summed_slots(sum_a)
    copies_b = exchange(sum_b, inner, peers_b, b_send, b_recv)
    for copy in row_copies + id_copies + forward + part_copies + copies_a:
        copy.wait_send()
    for copy in copies_b:
        copy.wait_recv()
    both = summed_slots(sum_b)
    mean_out[...] = jnp.sum(both[0:1, :], axis=1, keepdims=True) / jnp.sum(
        both[1:2, :], axis=1, keepdims=True
    )
    for copy in copies_b:
        copy.wait_send()


def build(dims, chunk):
    def shards(user, positive, row_ids, weights, offsets, neg, neg_ids):
        tokens, width = user.shape
        negs = neg.shape[0]
        tile, lines = tokens // TILES, tokens // 128
        ny, nz, nc = dims
        size_a, size_b = ny * NEG, nz * nc
        in_any = pl.BlockSpec(memory_space=pl.ANY)
        in_vmem = pl.BlockSpec(memory_space=pltpu.VMEM)
        dma = pltpu.SemaphoreType.DMA
        f32, bf16, i32 = jnp.float32, jnp.bfloat16, jnp.int32
        flops = 2 * NEG * tokens * negs * width
        loss, mean = pl.pallas_call(
            functools.partial(kernel, dims, chunk, 3.0 / math.sqrt(width) * LOG2E),
            out_shape=(
                jax.ShapeDtypeStruct((lines, 128), f32),
                jax.ShapeDtypeStruct((1, 1), f32),
            ),
            in_specs=[in_any] * 7,
            out_specs=(in_vmem, in_vmem),
            scratch_shapes=[
                pltpu.VMEM((STEPS * tile, width), bf16),
                pltpu.VMEM((STEPS, 1, tile), i32),
                pltpu.VMEM((tokens, width), bf16),
                pltpu.VMEM((negs, width), bf16),
                pltpu.VMEM((negs, 128), i32),
                pltpu.VMEM((STEPS, 1, tile), f32),
                pltpu.VMEM((NEG, TILES, 1, tile), f32),
                pltpu.VMEM((size_a, 2, 128), f32),
                pltpu.VMEM((size_b, 2, 128), f32),
                pltpu.VMEM((lines, 128), i32),
                pltpu.VMEM((lines, 128), i32),
                pltpu.VMEM((negs // 128, 128), i32),
                pltpu.SMEM(offsets.shape, i32),
                dma((7,)), dma((6,)), dma((4,)), dma((13,)), dma((9,)), dma((12,)),
                dma((9,)), dma((9,)),
                dma((size_a,)), dma((size_a,)), dma((size_b,)), dma((size_b,)),
            ],
            compiler_params=pltpu.CompilerParams(
                collective_id=0,
                has_side_effects=True,
            ),
            cost_estimate=pl.CostEstimate(
                flops=flops, bytes_accessed=2 * negs * width, transcendentals=0
            ),
        )(
            user, positive, row_ids.reshape(lines, 128), weights.reshape(lines, 128),
            offsets, neg, neg_ids.reshape(negs // 128, 128),
        )
        return loss.reshape(tokens), mean.reshape(())

    return shards


def on_mesh(mesh, dims, chunk):
    both = ("dp", "neg")
    return jax.shard_map(
        build(dims, chunk),
        mesh=mesh,
        in_specs=(
            P(both, None), P(both, None), P(both), P(both), P("dp", None),
            P("neg", None), P("neg"),
        ),
        out_specs=(P(both), P()),
        check_vma=False,
    )


def solution(mesh):
    return on_mesh(mesh, (4, 8, 2), 512)
```

```python
import functools
import math

import jax
import jax.numpy as jnp
from jax import lax
from jax.experimental import pallas as pl
from jax.experimental.pallas import tpu as pltpu
from jax.sharding import PartitionSpec as P

MESH = pl.DeviceIdType.MESH
LOG2E = math.log2(math.e)
LN2 = math.log(2.0)
MASKED = -1e30
FLOOR = -1e20
NEG = 4
TILES = 3
STEPS = NEG * TILES
BLOCK = 128
FROM_LEFT = {0: 3, 1: 5, 2: 7}
FROM_RIGHT = {2: 4, 1: 6, 0: 8}
FROM_FAR = {0: 9, 2: 10, 1: 11}


def nt_dot(a, b):
    return lax.dot_general(a, b, (((1,), (1,)), ((), ())), preferred_element_type=jnp.float32)


def in_pairs(parts):
    return (parts[0] + parts[2]) + (parts[1] + parts[3])


def kernel(
    dims, chunk, scale2,
    user, positive, row_ids, weights, offsets, neg, neg_ids,
    loss_out, mean_out,
    rows_v, ids_v, pos_v, neg_v, nid_v, part, scores, sum_b,
    id_rows, weight_rows, nid_rows, ends,
    load_sem, row_send, fwd_send, row_recv, id_send, id_recv, part_send, part_recv,
    weight_send, weight_recv, score_send, score_recv,
    b_send, b_recv,
):
    ny, nz, nc = dims
    per_y = nz * nc
    n = lax.axis_index("neg")
    d = lax.axis_index("dp")
    y, inner = d // per_y, d % per_y
    z, core = inner // nc, inner % nc
    right, left, far = (n + 1) % NEG, (n + 3) % NEG, (n + 2) % NEG
    tile = rows_v.shape[0] // STEPS
    half = tile // 2
    halves = tile // 128
    tokens = TILES * tile
    negs = neg_v.shape[0]

    peers_x = [(k, d, (n + k) % NEG) for k in range(1, NEG)]
    peers_b = [
        (
            k,
            ((y + k // per_y) % ny) * per_y
            + ((z + k % per_y // nc) % nz) * nc
            + (core + k % nc) % nc,
            n,
        )
        for k in range(1, ny * per_y)
    ]

    own = rows_v.at[pl.ds(0, tokens), :]
    pairs = (
        (neg_ids, nid_rows), (row_ids, id_rows), (user, own), (neg, neg_v),
        (positive, pos_v), (weights, weight_rows.at[0]), (offsets, ends),
    )
    loads = [
        pltpu.make_async_copy(src, dst, load_sem.at[k]) for k, (src, dst) in enumerate(pairs)
    ]
    for load in loads:
        load.start()

    barrier = pltpu.get_barrier_semaphore()
    for _, dp_to, neg_to in peers_x + peers_b:
        pl.semaphore_signal(barrier, inc=1, device_id=(dp_to, neg_to), device_id_type=MESH)

    loads[0].wait()
    loads[1].wait()
    for j in range(TILES):
        for h in range(halves):
            row = j * halves + h
            ids_v[j, :, h * 128 : (h + 1) * 128] = id_rows[row : row + 1, :]
    for r in range(negs // 128):
        nid_v[r * 128 : (r + 1) * 128, :] = jnp.broadcast_to(
            nid_rows[r : r + 1, :], (128, 128)
        ).T
    loads[2].wait()

    def rows_at(step, start=0, size=None):
        return rows_v.at[pl.ds(step * tile + start, size or tile), :]

    def remote(src, dst, send, recv, to):
        return pltpu.make_async_remote_copy(
            src_ref=src, dst_ref=dst, send_sem=send, recv_sem=recv,
            device_id=(d, to), device_id_type=MESH,
        )

    def id_copy(index, j, step, to):
        return remote(ids_v.at[j], ids_v.at[step], id_send.at[index], id_recv.at[step], to)

    def row_copy(index, j, step, to):
        return remote(rows_at(j), rows_at(step), row_send.at[index], row_recv.at[step], to)

    def swap(buffer, send, recv):
        return [
            remote(buffer.at[0], buffer.at[k], send.at[k], recv.at[k], to) for k, _, to in peers_x
        ]

    id_copies, row_copies = [], []
    for j in range(TILES):
        for table, to in ((FROM_LEFT, right), (FROM_RIGHT, left), (FROM_FAR, far)):
            id_copies.append(id_copy(len(id_copies), j, table[j], to))
    for jr, jl in ((0, 2), (1, 1), (2, 0)):
        row_copies.append(row_copy(len(row_copies), jr, FROM_LEFT[jr], right))
        row_copies.append(row_copy(len(row_copies), jl, FROM_RIGHT[jl], left))
    weight_copies = swap(weight_rows, weight_send, weight_recv)
    positive_copies = swap(scores, score_send, score_recv)
    part_copies = swap(part, part_send, part_recv)

    forward = [
        remote(rows_at(3), rows_at(9), fwd_send.at[0], row_recv.at[9], right),
        remote(rows_at(4), rows_at(10), fwd_send.at[1], row_recv.at[10], left),
        remote(rows_at(5, 0, half), rows_at(11, 0, half), fwd_send.at[2], row_recv.at[11], right),
        remote(
            rows_at(6, half, half), rows_at(11, half, half), fwd_send.at[3], row_recv.at[12], left
        ),
    ]
    for load in loads[4:]:
        load.wait()
    ones = jnp.ones((8, rows_v.shape[1]), jnp.bfloat16)
    for j in range(TILES):
        product = rows_v[j * tile : (j + 1) * tile, :].astype(jnp.float32) * pos_v[
            j * tile : (j + 1) * tile, :
        ].astype(jnp.float32)
        high = product.astype(jnp.bfloat16)
        low = (product - high.astype(jnp.float32)).astype(jnp.bfloat16)
        score = (nt_dot(ones, high) + nt_dot(ones, low))[0:1, :] * scale2
        for h in range(halves):
            row = j * halves + h
            scores[0, row : row + 1, :] = score[:, h * 128 : (h + 1) * 128]

    loads[3].wait()

    def one_tile(s, carry):
        @pl.when(s == 1)
        def _():
            pl.semaphore_wait(barrier, len(peers_x) + len(peers_b))
            for copy in id_copies + row_copies + weight_copies + positive_copies:
                copy.start()

        @pl.when(jnp.logical_and(s >= 3, s < 11))
        def _():
            remote(rows_at(0), rows_at(s), row_send.at[0], row_recv.at[s], right).wait_recv()

        @pl.when(s >= 3)
        def _():
            remote(ids_v.at[0], ids_v.at[s], id_send.at[0], id_recv.at[s], right).wait_recv()

        @pl.when(s == 11)
        def _():
            forward[2].wait_recv()
            forward[3].wait_recv()

        @pl.when(s == 4)
        def _():
            forward[0].start()
            forward[1].start()

        @pl.when(s == 6)
        def _():
            forward[2].start()
            forward[3].start()

        u = rows_v.at[pl.ds(pl.multiple_of(s * tile, tile), tile), :]
        rid = [ids_v[s, :, h * 128 : (h + 1) * 128] for h in range(halves)]

        state = [
            (jnp.full((8, 128), FLOOR, jnp.float32), jnp.zeros((8, 128), jnp.float32))
            for _ in range(halves)
        ]
        for c in range(negs // chunk):
            logits = nt_dot(neg_v[c * chunk : (c + 1) * chunk, :], u[...])
            for b in range(0, chunk, BLOCK):
                at = c * chunk + b
                for h in range(halves):
                    x = logits[b : b + BLOCK, h * 128 : (h + 1) * 128] * scale2
                    x = jnp.where(nid_v[at : at + BLOCK, :] == rid[h], MASKED, x)
                    x = x.reshape(BLOCK // 8, 8, 128)
                    peak, total = state[h]
                    new = jnp.maximum(peak, jnp.max(x, axis=0))
                    e = jnp.sum(jnp.exp2(x - new[None]), axis=0)
                    state[h] = (new, total * jnp.exp2(peak - new) + e)
        for h, (peak, total) in enumerate(state):
            top = jnp.max(peak, axis=0, keepdims=True)
            total = jnp.sum(total * jnp.exp2(peak - top), axis=0, keepdims=True)
            value = jnp.where(total > 0.0, top + jnp.log2(jnp.maximum(total, 1e-37)), MASKED)
            part[0, s, :, h * 128 : (h + 1) * 128] = value
        return carry

    lax.fori_loop(0, STEPS, one_tile, 0)

    for copy in part_copies:
        copy.start()
    for copy in weight_copies + positive_copies:
        copy.wait_recv()

    lane = lax.broadcasted_iota(jnp.int32, (1, 128), 1)
    alive = {}
    for k in range(NEG):
        owner = (n + NEG - k) % NEG
        for row in range(TILES * halves):
            place = owner * tokens + row * 128 + lane
            live = place < ends[0, ends.shape[1] - 1]
            for user_end in range(1, ends.shape[1]):
                live = jnp.logical_and(live, place + 1 != ends[0, user_end])
            alive[k, row] = jnp.where(live, 1.0, 0.0)

    for copy in part_copies:
        copy.wait_recv()
    totals, counts = [], []
    tables = [{0: 0, 1: 1, 2: 2}, FROM_LEFT, FROM_FAR, FROM_RIGHT]
    for k in range(NEG):
        total = jnp.zeros((1, 128), jnp.float32)
        count = jnp.zeros((1, 128), jnp.float32)
        for j in range(TILES):
            for h in range(halves):
                row = j * halves + h
                cut = slice(h * 128, (h + 1) * 128)
                pos2 = scores[k, row : row + 1, :]
                terms = [part[m, tables[(k - m) % NEG][j], :, cut] for m in range(NEG)]
                top = functools.reduce(jnp.maximum, terms, pos2)
                summed = in_pairs([jnp.exp2(term - top) for term in terms])
                summed = summed + jnp.exp2(pos2 - top)
                loss = jnp.where(
                    alive[k, row] > 0.0, (top - pos2 + jnp.log2(summed)) * LN2, 0.0
                )
                if k == 0:
                    loss_out[row : row + 1, :] = loss
                weight = weight_rows[k, row : row + 1, :].astype(jnp.float32)
                total = total + weight * loss
                count = count + weight * alive[k, row]
        totals.append(total)
        counts.append(count)

    def exchange(buffer, mine, peers, send, recv):
        copies = [
            pltpu.make_async_remote_copy(
                src_ref=buffer.at[mine], dst_ref=buffer.at[mine], send_sem=send.at[k],
                recv_sem=recv.at[k], device_id=(dp_to, neg_to), device_id_type=MESH,
            )
            for k, dp_to, neg_to in peers
        ]
        for copy in copies:
            copy.start()
        return copies

    def summed_slots(buffer):
        parts = [buffer[k] for k in range(buffer.shape[0])]
        while len(parts) > 1:
            parts = [a + b for a, b in zip(parts[::2], parts[1::2])]
        return parts[0]

    sum_b[d, 0:1, :] = in_pairs(totals)
    sum_b[d, 1:2, :] = in_pairs(counts)
    copies_b = exchange(sum_b, d, peers_b, b_send, b_recv)
    for copy in row_copies + id_copies + forward:
        copy.wait_send()
    for copy in weight_copies + positive_copies + part_copies:
        copy.wait_send()
    for copy in copies_b:
        copy.wait_recv()
    both = summed_slots(sum_b)
    mean_out[...] = jnp.sum(both[0:1, :], axis=1, keepdims=True) / jnp.sum(
        both[1:2, :], axis=1, keepdims=True
    )
    for copy in copies_b:
        copy.wait_send()


def build(dims, chunk):
    def shards(user, positive, row_ids, weights, offsets, neg, neg_ids):
        tokens, width = user.shape
        negs = neg.shape[0]
        tile, lines = tokens // TILES, tokens // 128
        ny, nz, nc = dims
        size_b = ny * nz * nc
        in_any = pl.BlockSpec(memory_space=pl.ANY)
        in_vmem = pl.BlockSpec(memory_space=pltpu.VMEM)
        dma = pltpu.SemaphoreType.DMA
        f32, bf16, i32 = jnp.float32, jnp.bfloat16, jnp.int32
        flops = 2 * NEG * tokens * negs * width
        loss, mean = pl.pallas_call(
            functools.partial(kernel, dims, chunk, 3.0 / math.sqrt(width) * LOG2E),
            out_shape=(
                jax.ShapeDtypeStruct((lines, 128), f32),
                jax.ShapeDtypeStruct((1, 1), f32),
            ),
            in_specs=[in_any] * 7,
            out_specs=(in_vmem, in_vmem),
            scratch_shapes=[
                pltpu.VMEM((STEPS * tile, width), bf16),
                pltpu.VMEM((STEPS, 1, tile), i32),
                pltpu.VMEM((tokens, width), bf16),
                pltpu.VMEM((negs, width), bf16),
                pltpu.VMEM((negs, 128), i32),
                pltpu.VMEM((NEG, STEPS, 1, tile), f32),
                pltpu.VMEM((NEG, lines, 128), f32),
                pltpu.VMEM((size_b, 2, 128), f32),
                pltpu.VMEM((lines, 128), i32),
                pltpu.VMEM((NEG, lines, 128), i32),
                pltpu.VMEM((negs // 128, 128), i32),
                pltpu.SMEM(offsets.shape, i32),
                dma((7,)), dma((6,)), dma((4,)), dma((13,)), dma((9,)), dma((12,)),
                dma((NEG,)), dma((NEG,)), dma((NEG,)), dma((NEG,)), dma((NEG,)), dma((NEG,)),
                dma((size_b,)), dma((size_b,)),
            ],
            compiler_params=pltpu.CompilerParams(
                collective_id=0,
                has_side_effects=True,
            ),
            cost_estimate=pl.CostEstimate(
                flops=flops, bytes_accessed=2 * negs * width, transcendentals=0
            ),
        )(
            user, positive, row_ids.reshape(lines, 128), weights.reshape(lines, 128),
            offsets, neg, neg_ids.reshape(negs // 128, 128),
        )
        return loss.reshape(tokens), mean.reshape(())

    return shards


def on_mesh(mesh, dims, chunk):
    both = ("dp", "neg")
    return jax.shard_map(
        build(dims, chunk),
        mesh=mesh,
        in_specs=(
            P(both, None), P(both, None), P(both), P(both), P("dp", None),
            P("neg", None), P("neg"),
        ),
        out_specs=(P(both), P()),
        check_vma=False,
    )


def solution(mesh):
    return on_mesh(mesh, (4, 8, 2), 512)
```

```python
import functools
import math

import jax
import jax.numpy as jnp
from jax import lax
from jax.experimental import pallas as pl
from jax.experimental.pallas import tpu as pltpu
from jax.sharding import PartitionSpec as P

MESH = pl.DeviceIdType.MESH
LOG2E = math.log2(math.e)
LN2 = math.log(2.0)
MASKED = -1e30
FLOOR = -1e20
NEG = 4
TILES = 3
STEPS = NEG * TILES
BLOCK = 128
FROM_LEFT = {0: 3, 1: 5, 2: 7}
FROM_RIGHT = {2: 4, 1: 6, 0: 8}
FROM_FAR = {0: 9, 2: 10, 1: 11}


def nt_dot(a, b):
    return lax.dot_general(a, b, (((1,), (1,)), ((), ())), preferred_element_type=jnp.float32)


def in_pairs(parts):
    return (parts[0] + parts[2]) + (parts[1] + parts[3])


def kernel(
    dims, chunk, scale2,
    user, positive, row_ids, weights, offsets, neg, neg_ids,
    loss_out, mean_out,
    rows_v, ids_v, pos_v, neg_v, nid_v, part, scores, sum_b,
    id_rows, weight_rows, nid_rows, ends,
    load_sem, row_send, fwd_send, row_recv, id_send, id_recv, part_send, part_recv,
    weight_send, weight_recv, score_send, score_recv,
    b_send, b_recv,
):
    ny, nz, nc = dims
    per_y = nz * nc
    n = lax.axis_index("neg")
    d = lax.axis_index("dp")
    y, inner = d // per_y, d % per_y
    z, core = inner // nc, inner % nc
    right, left, far = (n + 1) % NEG, (n + 3) % NEG, (n + 2) % NEG
    tile = rows_v.shape[0] // STEPS
    half = tile // 2
    halves = tile // 128
    tokens = TILES * tile
    negs = neg_v.shape[0]

    peers_x = [(k, d, (n + k) % NEG) for k in range(1, NEG)]
    peers_b = [
        (
            k,
            ((y + k // per_y) % ny) * per_y
            + ((z + k % per_y // nc) % nz) * nc
            + (core + k % nc) % nc,
            n,
        )
        for k in range(1, ny * per_y)
    ]

    own = rows_v.at[pl.ds(0, tokens), :]
    pairs = (
        (neg_ids, nid_rows), (row_ids, id_rows), (user, own), (positive, pos_v),
        (weights, weight_rows.at[0]), (offsets, ends), (neg, neg_v),
    )
    loads = [
        pltpu.make_async_copy(src, dst, load_sem.at[k]) for k, (src, dst) in enumerate(pairs)
    ]
    for load in loads:
        load.start()

    barrier = pltpu.get_barrier_semaphore()
    for _, dp_to, neg_to in peers_x + peers_b:
        pl.semaphore_signal(barrier, inc=1, device_id=(dp_to, neg_to), device_id_type=MESH)

    loads[0].wait()
    loads[1].wait()
    for j in range(TILES):
        for h in range(halves):
            row = j * halves + h
            ids_v[j, :, h * 128 : (h + 1) * 128] = id_rows[row : row + 1, :]
    for r in range(negs // 128):
        nid_v[r * 128 : (r + 1) * 128, :] = jnp.broadcast_to(
            nid_rows[r : r + 1, :], (128, 128)
        ).T
    loads[2].wait()

    def rows_at(step, start=0, size=None):
        return rows_v.at[pl.ds(step * tile + start, size or tile), :]

    def remote(src, dst, send, recv, to):
        return pltpu.make_async_remote_copy(
            src_ref=src, dst_ref=dst, send_sem=send, recv_sem=recv,
            device_id=(d, to), device_id_type=MESH,
        )

    def id_copy(index, j, step, to):
        return remote(ids_v.at[j], ids_v.at[step], id_send.at[index], id_recv.at[step], to)

    def row_copy(index, j, step, to):
        return remote(rows_at(j), rows_at(step), row_send.at[index], row_recv.at[step], to)

    def swap(buffer, send, recv):
        return [
            remote(buffer.at[0], buffer.at[k], send.at[k], recv.at[k], to) for k, _, to in peers_x
        ]

    id_copies, row_copies = [], []
    for j in range(TILES):
        for table, to in ((FROM_LEFT, right), (FROM_RIGHT, left), (FROM_FAR, far)):
            id_copies.append(id_copy(len(id_copies), j, table[j], to))
    for jr, jl in ((0, 2), (1, 1), (2, 0)):
        row_copies.append(row_copy(len(row_copies), jr, FROM_LEFT[jr], right))
        row_copies.append(row_copy(len(row_copies), jl, FROM_RIGHT[jl], left))
    weight_copies = swap(weight_rows, weight_send, weight_recv)
    positive_copies = swap(scores, score_send, score_recv)
    part_copies = swap(part, part_send, part_recv)

    forward = [
        remote(rows_at(3), rows_at(9), fwd_send.at[0], row_recv.at[9], right),
        remote(rows_at(4), rows_at(10), fwd_send.at[1], row_recv.at[10], left),
        remote(rows_at(5, 0, half), rows_at(11, 0, half), fwd_send.at[2], row_recv.at[11], right),
        remote(
            rows_at(6, half, half), rows_at(11, half, half), fwd_send.at[3], row_recv.at[12], left
        ),
    ]
    for load in loads[3:6]:
        load.wait()
    ones = jnp.ones((8, rows_v.shape[1]), jnp.bfloat16)
    for j in range(TILES):
        product = rows_v[j * tile : (j + 1) * tile, :].astype(jnp.float32) * pos_v[
            j * tile : (j + 1) * tile, :
        ].astype(jnp.float32)
        high = product.astype(jnp.bfloat16)
        low = (product - high.astype(jnp.float32)).astype(jnp.bfloat16)
        score = (nt_dot(ones, high) + nt_dot(ones, low))[0:1, :] * scale2
        for h in range(halves):
            row = j * halves + h
            scores[0, row : row + 1, :] = score[:, h * 128 : (h + 1) * 128]

    loads[6].wait()

    def one_tile(s, carry):
        @pl.when(s == 1)
        def _():
            pl.semaphore_wait(barrier, len(peers_x) + len(peers_b))
            for copy in id_copies + row_copies + weight_copies + positive_copies:
                copy.start()

        @pl.when(jnp.logical_and(s >= 3, s < 11))
        def _():
            remote(rows_at(0), rows_at(s), row_send.at[0], row_recv.at[s], right).wait_recv()

        @pl.when(s >= 3)
        def _():
            remote(ids_v.at[0], ids_v.at[s], id_send.at[0], id_recv.at[s], right).wait_recv()

        @pl.when(s == 11)
        def _():
            forward[2].wait_recv()
            forward[3].wait_recv()

        @pl.when(s == 4)
        def _():
            forward[0].start()
            forward[1].start()

        @pl.when(s == 6)
        def _():
            forward[2].start()
            forward[3].start()

        u = rows_v.at[pl.ds(pl.multiple_of(s * tile, tile), tile), :]
        rid = [ids_v[s, :, h * 128 : (h + 1) * 128] for h in range(halves)]

        state = [
            (jnp.full((8, 128), FLOOR, jnp.float32), jnp.zeros((8, 128), jnp.float32))
            for _ in range(halves)
        ]
        for c in range(negs // chunk):
            logits = nt_dot(neg_v[c * chunk : (c + 1) * chunk, :], u[...])
            for b in range(0, chunk, BLOCK):
                at = c * chunk + b
                for h in range(halves):
                    x = logits[b : b + BLOCK, h * 128 : (h + 1) * 128] * scale2
                    x = jnp.where(nid_v[at : at + BLOCK, :] == rid[h], MASKED, x)
                    x = x.reshape(BLOCK // 8, 8, 128)
                    peak, total = state[h]
                    new = jnp.maximum(peak, jnp.max(x, axis=0))
                    e = jnp.sum(jnp.exp2(x - new[None]), axis=0)
                    state[h] = (new, total * jnp.exp2(peak - new) + e)
        for h, (peak, total) in enumerate(state):
            top = jnp.max(peak, axis=0, keepdims=True)
            total = jnp.sum(total * jnp.exp2(peak - top), axis=0, keepdims=True)
            value = jnp.where(total > 0.0, top + jnp.log2(jnp.maximum(total, 1e-37)), MASKED)
            part[0, s, :, h * 128 : (h + 1) * 128] = value
        return carry

    lax.fori_loop(0, STEPS, one_tile, 0)

    for copy in part_copies:
        copy.start()
    for copy in weight_copies + positive_copies:
        copy.wait_recv()

    lane = lax.broadcasted_iota(jnp.int32, (1, 128), 1)
    alive = {}
    for k in range(NEG):
        owner = (n + NEG - k) % NEG
        for row in range(TILES * halves):
            place = owner * tokens + row * 128 + lane
            live = place < ends[0, ends.shape[1] - 1]
            for user_end in range(1, ends.shape[1]):
                live = jnp.logical_and(live, place + 1 != ends[0, user_end])
            alive[k, row] = jnp.where(live, 1.0, 0.0)

    for copy in part_copies:
        copy.wait_recv()
    totals, counts = [], []
    tables = [{0: 0, 1: 1, 2: 2}, FROM_LEFT, FROM_FAR, FROM_RIGHT]
    for k in range(NEG):
        total = jnp.zeros((1, 128), jnp.float32)
        count = jnp.zeros((1, 128), jnp.float32)
        for j in range(TILES):
            for h in range(halves):
                row = j * halves + h
                cut = slice(h * 128, (h + 1) * 128)
                pos2 = scores[k, row : row + 1, :]
                terms = [part[m, tables[(k - m) % NEG][j], :, cut] for m in range(NEG)]
                top = functools.reduce(jnp.maximum, terms, pos2)
                summed = in_pairs([jnp.exp2(term - top) for term in terms])
                summed = summed + jnp.exp2(pos2 - top)
                loss = jnp.where(
                    alive[k, row] > 0.0, (top - pos2 + jnp.log2(summed)) * LN2, 0.0
                )
                if k == 0:
                    loss_out[row : row + 1, :] = loss
                weight = weight_rows[k, row : row + 1, :].astype(jnp.float32)
                total = total + weight * loss
                count = count + weight * alive[k, row]
        totals.append(total)
        counts.append(count)

    def exchange(buffer, mine, peers, send, recv):
        copies = [
            pltpu.make_async_remote_copy(
                src_ref=buffer.at[mine], dst_ref=buffer.at[mine], send_sem=send.at[k],
                recv_sem=recv.at[k], device_id=(dp_to, neg_to), device_id_type=MESH,
            )
            for k, dp_to, neg_to in peers
        ]
        for copy in copies:
            copy.start()
        return copies

    def summed_slots(buffer):
        parts = [buffer[k] for k in range(buffer.shape[0])]
        while len(parts) > 1:
            parts = [a + b for a, b in zip(parts[::2], parts[1::2])]
        return parts[0]

    sum_b[d, 0:1, :] = in_pairs(totals)
    sum_b[d, 1:2, :] = in_pairs(counts)
    copies_b = exchange(sum_b, d, peers_b, b_send, b_recv)
    for copy in row_copies + id_copies + forward:
        copy.wait_send()
    for copy in weight_copies + positive_copies + part_copies:
        copy.wait_send()
    for copy in copies_b:
        copy.wait_recv()
    both = summed_slots(sum_b)
    mean_out[...] = jnp.sum(both[0:1, :], axis=1, keepdims=True) / jnp.sum(
        both[1:2, :], axis=1, keepdims=True
    )
    for copy in copies_b:
        copy.wait_send()


def build(dims, chunk):
    def shards(user, positive, row_ids, weights, offsets, neg, neg_ids):
        tokens, width = user.shape
        negs = neg.shape[0]
        tile, lines = tokens // TILES, tokens // 128
        ny, nz, nc = dims
        size_b = ny * nz * nc
        in_any = pl.BlockSpec(memory_space=pl.ANY)
        in_vmem = pl.BlockSpec(memory_space=pltpu.VMEM)
        dma = pltpu.SemaphoreType.DMA
        f32, bf16, i32 = jnp.float32, jnp.bfloat16, jnp.int32
        flops = 2 * NEG * tokens * negs * width
        loss, mean = pl.pallas_call(
            functools.partial(kernel, dims, chunk, 3.0 / math.sqrt(width) * LOG2E),
            out_shape=(
                jax.ShapeDtypeStruct((lines, 128), f32),
                jax.ShapeDtypeStruct((1, 1), f32),
            ),
            in_specs=[in_any] * 7,
            out_specs=(in_vmem, in_vmem),
            scratch_shapes=[
                pltpu.VMEM((STEPS * tile, width), bf16),
                pltpu.VMEM((STEPS, 1, tile), i32),
                pltpu.VMEM((tokens, width), bf16),
                pltpu.VMEM((negs, width), bf16),
                pltpu.VMEM((negs, 128), i32),
                pltpu.VMEM((NEG, STEPS, 1, tile), f32),
                pltpu.VMEM((NEG, lines, 128), f32),
                pltpu.VMEM((size_b, 2, 128), f32),
                pltpu.VMEM((lines, 128), i32),
                pltpu.VMEM((NEG, lines, 128), i32),
                pltpu.VMEM((negs // 128, 128), i32),
                pltpu.SMEM(offsets.shape, i32),
                dma((7,)), dma((6,)), dma((4,)), dma((13,)), dma((9,)), dma((12,)),
                dma((NEG,)), dma((NEG,)), dma((NEG,)), dma((NEG,)), dma((NEG,)), dma((NEG,)),
                dma((size_b,)), dma((size_b,)),
            ],
            compiler_params=pltpu.CompilerParams(
                collective_id=0,
                has_side_effects=True,
            ),
            cost_estimate=pl.CostEstimate(
                flops=flops, bytes_accessed=2 * negs * width, transcendentals=0
            ),
        )(
            user, positive, row_ids.reshape(lines, 128), weights.reshape(lines, 128),
            offsets, neg, neg_ids.reshape(negs // 128, 128),
        )
        return loss.reshape(tokens), mean.reshape(())

    return shards


def on_mesh(mesh, dims, chunk):
    both = ("dp", "neg")
    return jax.shard_map(
        build(dims, chunk),
        mesh=mesh,
        in_specs=(
            P(both, None), P(both, None), P(both), P(both), P("dp", None),
            P("neg", None), P("neg"),
        ),
        out_specs=(P(both), P()),
        check_vma=False,
    )


def solution(mesh):
    return on_mesh(mesh, (4, 8, 2), 512)
```
